32 devices in a mesh: dp: 8 (over z, core), tensor: 4 (over y, x).
Axes of the slice: x: 2, y: 2, z: 4, core: 2. Of those that a mesh axis runs over, the one named last changes fastest.
Arguments:
- block_input: bfloat16 [2048, 5120], P('dp'), may hold values from -6 to 6
- query_weight: bfloat16 [2560, 5120], P('tensor'), as said below
- query_gain: float32 [2560], P('tensor'), may hold values from 0.5 to 2
- query_grad: bfloat16 [2560, 2048], P('tensor', 'dp'), may hold values from -6 to 6
Outputs:
- input_grad: bfloat16 [2048, 5120], P(('dp', 'tensor'))
- weight_grad: float32 [5120, 2560], P('dp', 'tensor')
The draws below stay inside these ranges and needn't reach their ends.
Inputs may be any that keep to these rules, and one draw needn't show every extreme that they name: `query_weight`: entries are normal with standard deviation 5120 ** -0.5 times a factor between 0.25 and 75, which may differ from row to row and from column to column.
All inputs are finite; a program needn't handle non-finite values.
Results may differ from the reference program's by a relative error of at most 0.017.
Values may be sent and summed in bfloat16 or wider, within the bound.
A program may use at most 64 MiB of HBM per device.

```python
import math
import jax
import jax.numpy as jnp
from jax import lax

D = 5120
HQ = 2560
TOKENS = 2048
N_TENSOR = 4


def draw_query_weight(key, part):
    first = jax.random.fold_in(key, 0)
    base = jax.random.normal(first, (HQ, D), jnp.float32) / math.sqrt(D)
    ramp = jnp.exp(math.log(3.0) * jnp.arange(HQ, dtype=jnp.float32) / HQ)[:, None]
    return (base * ramp).astype(jnp.bfloat16)


def strengthened(values, stream_key, source, target, shards_of, factor):
    def block_of(dim):
        return (jnp.arange(values.shape[dim]) // (values.shape[dim] // shards_of)).reshape((-1,) + (1,) * (values.ndim - 1 - dim))

    first = jax.random.permutation(stream_key, shards_of)[block_of(target)]
    far = (block_of(target) + shards_of // 2) % shards_of
    return jnp.where((block_of(source) == first) | (block_of(source) == far), factor * values, values)


def block_levels(rng, extent, shards, least, high):
    factor_of, own = 1.0, jax.random.fold_in(rng, 6)
    for position, parts in shards:
        steps = jnp.exp(jax.random.uniform(jax.random.fold_in(own, position), (parts,), jnp.float32, least / len(shards), high / len(shards)))
        factor_of = factor_of * jnp.repeat(steps, extent[position] // parts).reshape([-1 if axis == position else 1 for axis in range(len(extent))])
    return factor_of


def centred(key, shape, deviation, limit, cuts=(), held_as=jnp.bfloat16):
    factor_of = block_levels(key, shape, cuts, -0.22, 0.18) if cuts else 1.0
    result = jax.random.normal(key, shape, jnp.float32) * deviation * factor_of
    return jnp.minimum(jnp.maximum(result, -limit), limit).astype(held_as)


def heavy_noise(stream_key, dims, scale, most, cuts, heavy, kind=jnp.bfloat16):
    values = scale * jax.random.normal(stream_key, dims, jnp.float32)
    if cuts:
        values = values * block_levels(stream_key, dims, cuts, -0.22, 0.18)
    return jnp.clip(strengthened(values, jax.random.fold_in(stream_key, 3), *heavy), -most, most).astype(kind)


def setup_inputs(seed: int = 0) -> dict:
    splits = jax.random.split(jax.random.key(seed), 5)
    return {
        "block_input": heavy_noise(splits[0], (TOKENS, D), 1.0, 6.0, ((0, 8),), (0, 1, 8, 2.0)),
        "query_weight": draw_query_weight(jax.random.fold_in(splits[4], 71), 0),
        "query_gain": jnp.clip(jnp.exp(math.log(2.0) - 1.3862944 * jax.random.uniform(splits[2], (HQ,), jnp.float32) ** block_levels(splits[2], (HQ,), ((0, 4),), -0.2, 0.2)), 0.5, 2.0),
        "query_grad": centred(splits[3], (HQ, TOKENS), 1.0, 6.0, ((0, 4), (1, 8))),
    }


epsilon = 1e-06

def reference(block_input, query_weight, query_gain, query_grad):
    projected = jnp.dot(block_input, query_weight.T, preferred_element_type=jnp.float32)
    squares = lax.optimization_barrier(jnp.sum(projected * projected, axis=1, keepdims=True))
    inverse_rms = 1.0 / jnp.sqrt(squares / HQ + epsilon)
    scaled_grad = query_grad.T.astype(jnp.float32) * query_gain
    cross_sums = lax.optimization_barrier(jnp.sum(scaled_grad * projected, axis=1, keepdims=True))
    coefficient = inverse_rms * inverse_rms * inverse_rms * (cross_sums / HQ)
    proj_grad = (inverse_rms * scaled_grad - coefficient * projected).astype(jnp.bfloat16)
    group = HQ // N_TENSOR
    total = jnp.zeros((TOKENS, D), jnp.float32)
    for member in range(N_TENSOR):
        lower = member * group
        term = jnp.dot(proj_grad[:, lower:lower + group], query_weight[lower:lower + group, :], preferred_element_type=jnp.float32)
        rounded = lax.optimization_barrier(term.astype(jnp.bfloat16)).astype(jnp.float32)
        total = total + rounded
    input_grad = total.astype(jnp.bfloat16)
    weight_grad = jnp.dot(block_input.T, proj_grad, preferred_element_type=jnp.float32)
    return (input_grad, weight_grad)
```

```python
import functools

import jax
import jax.numpy as jnp
from jax import lax
from jax.experimental import pallas as pl
from jax.experimental.pallas import tpu as pltpu
from jax.sharding import PartitionSpec as P

epsilon = 1e-06
MESH = pl.DeviceIdType.MESH


def plain(block_input, query_weight, query_gain, query_grad):
    projected = lax.dot_general(
        query_weight, block_input, (((1,), (1,)), ((), ())), preferred_element_type=jnp.float32
    )
    scaled_grad = query_grad.astype(jnp.float32) * query_gain[:, None]
    squares = jnp.sum(projected * projected, axis=0)
    cross_sums = jnp.sum(scaled_grad * projected, axis=0)
    features = query_gain.shape[0] * lax.axis_size("tensor")
    squares, cross_sums = lax.psum((squares, cross_sums), "tensor")
    inverse_rms = 1.0 / jnp.sqrt(squares / features + epsilon)
    coefficient = inverse_rms * inverse_rms * inverse_rms * (cross_sums / features)
    proj_grad = (inverse_rms[None, :] * scaled_grad - coefficient[None, :] * projected).astype(
        jnp.bfloat16
    )
    input_grad = lax.psum_scatter(
        lax.dot_general(
            proj_grad, query_weight, (((0,), (0,)), ((), ())), preferred_element_type=jnp.float32
        ).astype(jnp.bfloat16),
        "tensor",
        scatter_dimension=0,
        tiled=True,
    )
    weight_grad = lax.psum_scatter(
        lax.dot_general(
            block_input, proj_grad, (((0,), (1,)), ((), ())), preferred_element_type=jnp.float32
        ),
        "dp",
        scatter_dimension=0,
        tiled=True,
    )
    return (input_grad, weight_grad)


def kernel(
    ndp, nt, fchunks, nchunks, near,
    x_hbm, w_hbm, qg_hbm, gain_ref,
    ig_ref, wg_ref,
    xv, wv, qv, sg, proj, stats, gt, gbuf, xbuf, part, rsbuf,
    lsem, wsem, st_s, st_r, xs, xr, fs, fr, gs, gr, rs_s, rs_r,
):
    tokens, width = xv.shape
    feats = wv.shape[0]
    cols = width // ndp
    rows = tokens // nt
    fstep = feats // fchunks
    nstep = width // nchunks
    nz = ndp // 2
    d = lax.axis_index("dp")
    t = lax.axis_index("tensor")
    z = d // 2
    c = d % 2
    partner = 2 * z + (1 - c)
    mine = pl.ds(pl.multiple_of(t * rows, rows), rows)

    def remote(src, dst, send, recv, dd, tt):
        return pltpu.make_async_remote_copy(
            src_ref=src, dst_ref=dst, send_sem=send, recv_sem=recv,
            device_id=(dd, tt), device_id_type=MESH,
        )

    x_load = pltpu.make_async_copy(x_hbm, xv, lsem.at[0])
    x_load.start()

    def w_load(i):
        r = pl.ds(i * fstep, fstep)
        return pltpu.make_async_copy(w_hbm.at[r], wv.at[r], wsem.at[i])

    for i in range(fchunks):
        w_load(i).start()
    q_load = pltpu.make_async_copy(qg_hbm, qv, lsem.at[1])
    q_load.start()

    barrier = pltpu.get_barrier_semaphore()
    for o in range(1, ndp):
        pl.semaphore_signal(barrier, inc=1, device_id=((d + o) % ndp, t), device_id_type=MESH)
    for o in range(1, nt):
        pl.semaphore_signal(barrier, inc=1, device_id=(d, (t + o) % nt), device_id_type=MESH)
    pl.semaphore_wait(barrier, ndp + nt - 2)

    def col_block(s):
        return pl.ds(pl.multiple_of(s * cols, cols), cols)

    def x_whole(s, dst_slot, recv_slot):
        return remote(
            x_hbm.at[:, col_block(s)], xbuf.at[dst_slot], xs.at[s], xr.at[recv_slot], s, t
        )

    def x_share(s, dst_slot, recv_slot):
        return remote(
            x_hbm.at[mine, col_block(s)], xbuf.at[dst_slot, mine], xs.at[s], xr.at[recv_slot], s, t
        )

    for zt in range(nz):
        @pl.when(jnp.abs(z - zt) > near)
        def _(zt=zt):
            for ct in range(2):
                x_share(2 * zt + ct, d, d).start()
    x_whole(partner, d, d).start()

    q_load.wait()
    grow = jnp.broadcast_to(gain_ref[...], (128, feats))
    gcol = jnp.transpose(grow)
    for k in range(tokens // 128):
        sl = pl.ds(k * 128, 128)
        sg[:, sl] = qv[:, sl].astype(jnp.float32) * gcol
    x_load.wait()
    sq = jnp.zeros((1, tokens), jnp.float32)
    cr = jnp.zeros((1, tokens), jnp.float32)
    for i in range(fchunks):
        w_load(i).wait()
        r = pl.ds(i * fstep, fstep)
        p = lax.dot_general(
            wv[r, :], xv[...], (((1,), (1,)), ((), ())), preferred_element_type=jnp.float32
        )
        proj[r, :] = p
        sq = sq + jnp.sum(p * p, axis=0, keepdims=True)
        cr = cr + jnp.sum(sg[r, :] * p, axis=0, keepdims=True)
    stats[t, 0:1, :] = sq
    stats[t, 1:2, :] = cr

    def stat_copy(o, slot):
        return remote(stats.at[t], stats.at[slot], st_s.at[o], st_r.at[o], d, (t + o) % nt)

    for o in range(1, nt):
        stat_copy(o, t).start()
    for o in range(1, nt):
        stat_copy(o, (t - o + nt) % nt).wait_recv()
    sq = stats[0, 0:1, :]
    cr = stats[0, 1:2, :]
    for k in range(1, nt):
        sq = sq + stats[k, 0:1, :]
        cr = cr + stats[k, 1:2, :]
    features = feats * nt
    inv = 1.0 / jnp.sqrt(sq / features + epsilon)
    coef = inv * inv * inv * (cr / features)
    gt[...] = inv * sg[...] - coef * proj[...]
    gbuf[d] = jnp.transpose(gt[...]).astype(jnp.bfloat16)

    def g_copy(way, s):
        dd = {0: d - 2, 1: d + 2, 2: partner}[way]
        return remote(gbuf.at[s], gbuf.at[s], gs.at[way, s], gr.at[s], dd, t)

    @pl.when(z > 0)
    def _():
        g_copy(0, d).start()

    @pl.when(z < nz - 1)
    def _():
        g_copy(1, d).start()

    g_copy(2, d).start()

    def x_near(ct):
        for zt in range(nz):
            @pl.when((jnp.abs(z - zt) <= near) & (z != zt))
            def _(zt=zt):
                x_whole(2 * zt + ct, d, d).start()

    x_near(0)

    def rs_copy(n, o, slot, who):
        sl = pl.ds(pl.multiple_of(n * nstep, nstep), nstep)
        rr = pl.ds(pl.multiple_of(who * rows, rows), rows)
        return remote(
            part.at[rr, sl], rsbuf.at[slot, :, sl], rs_s.at[n, o], rs_r.at[n, o], d, who
        )

    def share(n, carry):
        sl = pl.ds(pl.multiple_of(n * nstep, nstep), nstep)
        part[:, sl] = jnp.dot(
            gbuf[d], wv[:, sl], preferred_element_type=jnp.float32
        ).astype(jnp.bfloat16)
        for o in range(1, nt):
            rs_copy(n, o, o, (t + o) % nt).start()
        return carry

    lax.fori_loop(0, nchunks, share, 0)

    def f_copy(s, o):
        return remote(
            xbuf.at[s, mine], xbuf.at[s, mine], fs.at[s, o], fr.at[s, o], d, (t + o) % nt
        )

    def f_arrived(s, o):
        src = (t - o + nt) % nt
        there = pl.ds(pl.multiple_of(src * rows, rows), rows)
        return remote(
            xbuf.at[s, there], xbuf.at[s, there], fs.at[s, o], fr.at[s, o], d, (t + o) % nt
        )

    for dist in range(nz - 1, near, -1):
        for zs_of in (lambda: z - dist, lambda: z + dist):
            zs = zs_of()

            @pl.when((zs >= 0) & (zs < nz))
            def _(zs=zs):
                for cs in range(2):
                    s = 2 * zs + cs
                    x_share(d, s, s).wait_recv()
                    for o in range(1, nt):
                        f_copy(s, o).start()

    def chain(k):
        @pl.when(z - k >= 0)
        def _():
            s = 2 * (z - k) + c
            g_copy(1, s).wait_recv()

            @pl.when(z < nz - 1)
            def _():
                g_copy(1, s).start()

            g_copy(2, s).start()

        @pl.when(z + k < nz)
        def _():
            s = 2 * (z + k) + c
            g_copy(0, s).wait_recv()

            @pl.when(z > 0)
            def _():
                g_copy(0, s).start()

            g_copy(2, s).start()

    def accumulate(s):
        wg_ref[...] += lax.dot_general(
            xbuf[s], gbuf[s], (((0,), (0,)), ((), ())), preferred_element_type=jnp.float32
        )

    def weight_terms(k):
        def one(i, carry):
            zs = z + (2 * (i // 2) - 1) * k
            cs = i % 2

            @pl.when((zs >= 0) & (zs < nz))
            def _():
                s = 2 * zs + cs
                if k <= near:
                    x_whole(d, s, s).wait_recv()
                else:
                    for o in range(1, nt):
                        f_arrived(s, o).wait_recv()

                @pl.when(cs != c)
                def _():
                    g_copy(2, s).wait_recv()

                accumulate(s)

            return carry

        lax.fori_loop(0, 4, one, 0)

    own = pltpu.make_async_copy(x_hbm.at[:, col_block(d)], xbuf.at[d], lsem.at[2])
    own.start()
    chain(1)
    x_near(1)
    own.wait()
    wg_ref[...] = jnp.zeros_like(wg_ref)
    accumulate(d)
    x_whole(d, partner, partner).wait_recv()
    g_copy(2, partner).wait_recv()
    accumulate(partner)
    for k in range(2, nz):
        chain(k)
        weight_terms(k - 1)

    def total(n, carry):
        sl = pl.ds(pl.multiple_of(n * nstep, nstep), nstep)
        acc = part[mine, sl].astype(jnp.float32)
        for o in range(1, nt):
            rs_copy(n, o, o, t).wait_recv()
            acc = acc + rsbuf[o, :, sl].astype(jnp.float32)
        ig_ref[:, sl] = acc.astype(jnp.bfloat16)
        return carry

    lax.fori_loop(0, nchunks, total, 0)
    weight_terms(nz - 1)

    for o in range(1, nt):
        stat_copy(o, t).wait_send()
    for zt in range(nz):
        for ct in range(2):
            s = 2 * zt + ct

            @pl.when(jnp.abs(z - zt) > near)
            def _(s=s):
                x_share(s, d, d).wait_send()
                for o in range(1, nt):
                    f_copy(s, o).wait_send()

            @pl.when((jnp.abs(z - zt) <= near) & (z != zt))
            def _(s=s):
                x_whole(s, d, d).wait_send()

        s = 2 * zt + c

        @pl.when((zt >= z) & (z > 0))
        def _(s=s):
            g_copy(0, s).wait_send()

        @pl.when((zt <= z) & (z < nz - 1))
        def _(s=s):
            g_copy(1, s).wait_send()

        g_copy(2, s).wait_send()
    x_whole(partner, d, d).wait_send()

    def sent(n, carry):
        for o in range(1, nt):
            rs_copy(n, o, o, (t + o) % nt).wait_send()
        return carry

    lax.fori_loop(0, nchunks, sent, 0)


def fused(block_input, query_weight, query_gain, query_grad):
    ndp = lax.axis_size("dp")
    nt = lax.axis_size("tensor")
    tokens, width = block_input.shape
    feats = query_weight.shape[0]
    cols, rows = width // ndp, tokens // nt
    fchunks, nchunks = 2, 4
    dma = pltpu.SemaphoreType.DMA
    bf, f32 = jnp.bfloat16, jnp.float32
    any_spec = pl.BlockSpec(memory_space=pl.ANY)
    vmem = pl.BlockSpec(memory_space=pltpu.VMEM)
    return pl.pallas_call(
        functools.partial(kernel, ndp, nt, fchunks, nchunks, 1),
        out_shape=(
            jax.ShapeDtypeStruct((rows, width), bf),
            jax.ShapeDtypeStruct((cols, feats), f32),
        ),
        in_specs=[any_spec, any_spec, any_spec, vmem],
        out_specs=(vmem, vmem),
        scratch_shapes=[
            pltpu.VMEM((tokens, width), bf),
            pltpu.VMEM((feats, width), bf),
            pltpu.VMEM((feats, tokens), bf),
            pltpu.VMEM((feats, tokens), f32),
            pltpu.VMEM((feats, tokens), f32),
            pltpu.VMEM((nt, 8, tokens), f32),
            pltpu.VMEM((feats, tokens), f32),
            pltpu.VMEM((ndp, tokens, feats), bf),
            pltpu.VMEM((ndp, tokens, cols), bf),
            pltpu.VMEM((tokens, width), bf),
            pltpu.VMEM((nt, rows, width), bf),
            dma((3,)), dma((fchunks,)),
            dma((nt,)), dma((nt,)),
            dma((ndp,)), dma((ndp,)),
            dma((ndp, nt)), dma((ndp, nt)),
            dma((3, ndp)), dma((ndp,)),
            dma((nchunks, nt)), dma((nchunks, nt)),
        ],
        compiler_params=pltpu.CompilerParams(
            collective_id=0, has_side_effects=True, vmem_limit_bytes=56 * 1024 * 1024
        ),
        name="query_backward",
    )(block_input, query_weight, query_grad, query_gain.reshape(1, feats))


def per_device(block_input, query_weight, query_gain, query_grad):
    ndp = lax.axis_size("dp")
    nt = lax.axis_size("tensor")
    tokens, width = block_input.shape
    feats = query_weight.shape[0]
    aligned = (
        ndp % 2 == 0 and ndp >= 4 and nt >= 2
        and width % (128 * ndp) == 0 and width % (128 * 4) == 0
        and feats % 128 == 0 and tokens % 128 == 0 and tokens % (16 * nt) == 0
        and 2 * width * (feats + 4 * tokens) + 24 * tokens * feats < 40 * 2**20
    )
    body = fused if aligned else plain
    return body(block_input, query_weight, query_gain, query_grad)


def solution(mesh):
    in_specs = (P("dp", None), P("tensor", None), P("tensor"), P("tensor", "dp"))
    out_specs = (P(("dp", "tensor"), None), P("dp", "tensor"))
    return jax.shard_map(
        per_device, mesh=mesh, in_specs=in_specs, out_specs=out_specs, check_vma=False
    )
```

```python
import functools

import jax
import jax.numpy as jnp
from jax import lax
from jax.experimental import pallas as pl
from jax.experimental.pallas import tpu as pltpu
from jax.sharding import PartitionSpec as P

epsilon = 1e-06
MESH = pl.DeviceIdType.MESH


def plain(block_input, query_weight, query_gain, query_grad):
    projected = lax.dot_general(
        query_weight, block_input, (((1,), (1,)), ((), ())), preferred_element_type=jnp.float32
    )
    scaled_grad = query_grad.astype(jnp.float32) * query_gain[:, None]
    squares = jnp.sum(projected * projected, axis=0)
    cross_sums = jnp.sum(scaled_grad * projected, axis=0)
    features = query_gain.shape[0] * lax.axis_size("tensor")
    squares, cross_sums = lax.psum((squares, cross_sums), "tensor")
    inverse_rms = 1.0 / jnp.sqrt(squares / features + epsilon)
    coefficient = inverse_rms * inverse_rms * inverse_rms * (cross_sums / features)
    proj_grad = (inverse_rms[None, :] * scaled_grad - coefficient[None, :] * projected).astype(
        jnp.bfloat16
    )
    input_grad = lax.psum_scatter(
        lax.dot_general(
            proj_grad, query_weight, (((0,), (0,)), ((), ())), preferred_element_type=jnp.float32
        ).astype(jnp.bfloat16),
        "tensor",
        scatter_dimension=0,
        tiled=True,
    )
    weight_grad = lax.psum_scatter(
        lax.dot_general(
            block_input, proj_grad, (((0,), (1,)), ((), ())), preferred_element_type=jnp.float32
        ),
        "dp",
        scatter_dimension=0,
        tiled=True,
    )
    return (input_grad, weight_grad)


def kernel(
    ndp, nt, fchunks, nchunks, near,
    x_hbm, w_hbm, qg_hbm, gain_ref,
    ig_ref, wg_ref,
    xv, wv, qv, sg, proj, stats, gt, gbuf, xbuf, part, rsbuf, relay,
    lsem, wsem, st_s, st_r, xs, xr, fs, fr, gs, gr, rs_s, rs_r,
):
    tokens, width = xv.shape
    feats = wv.shape[0]
    cols = width // ndp
    rows = tokens // nt
    fstep = feats // fchunks
    nstep = width // nchunks
    nz = ndp // 2
    d = lax.axis_index("dp")
    t = lax.axis_index("tensor")
    z = d // 2
    c = d % 2
    partner = 2 * z + (1 - c)
    mine = pl.ds(pl.multiple_of(t * rows, rows), rows)

    def remote(src, dst, send, recv, dd, tt):
        return pltpu.make_async_remote_copy(
            src_ref=src, dst_ref=dst, send_sem=send, recv_sem=recv,
            device_id=(dd, tt), device_id_type=MESH,
        )

    x_load = pltpu.make_async_copy(x_hbm, xv, lsem.at[0])
    x_load.start()

    def w_load(i):
        r = pl.ds(i * fstep, fstep)
        return pltpu.make_async_copy(w_hbm.at[r], wv.at[r], wsem.at[i])

    for i in range(fchunks):
        w_load(i).start()
    q_load = pltpu.make_async_copy(qg_hbm, qv, lsem.at[1])
    q_load.start()

    barrier = pltpu.get_barrier_semaphore()
    for o in range(1, ndp):
        pl.semaphore_signal(barrier, inc=1, device_id=((d + o) % ndp, t), device_id_type=MESH)
    for o in range(1, nt):
        pl.semaphore_signal(barrier, inc=1, device_id=(d, (t + o) % nt), device_id_type=MESH)
    pl.semaphore_wait(barrier, ndp + nt - 2)

    def col_block(s):
        return pl.ds(pl.multiple_of(s * cols, cols), cols)

    def x_whole(s, dst_slot, recv_slot):
        return remote(
            x_hbm.at[:, col_block(s)], xbuf.at[dst_slot], xs.at[s], xr.at[recv_slot], s, t
        )

    def x_share(s, dst_slot, recv_slot):
        return remote(
            x_hbm.at[mine, col_block(s)], xbuf.at[dst_slot, mine], xs.at[s], xr.at[recv_slot], s, t
        )

    for zt in range(nz):
        @pl.when(jnp.abs(z - zt) > near)
        def _(zt=zt):
            for ct in range(2):
                x_share(2 * zt + ct, d, d).start()
    x_whole(partner, d, d).start()

    q_load.wait()
    grow = jnp.broadcast_to(gain_ref[...].reshape(1, feats), (128, feats))
    gcol = jnp.transpose(grow)
    for k in range(tokens // 128):
        sl = pl.ds(k * 128, 128)
        sg[:, sl] = qv[:, sl].astype(jnp.float32) * gcol
    x_load.wait()
    sq = jnp.zeros((1, tokens), jnp.float32)
    cr = jnp.zeros((1, tokens), jnp.float32)
    for i in range(fchunks):
        w_load(i).wait()
        r = pl.ds(i * fstep, fstep)
        p = lax.dot_general(
            wv[r, :], xv[...], (((1,), (1,)), ((), ())), preferred_element_type=jnp.float32
        )
        proj[r, :] = p
        sq = sq + jnp.sum(p * p, axis=0, keepdims=True)
        cr = cr + jnp.sum(sg[r, :] * p, axis=0, keepdims=True)
    stats[t, 0:1, :] = sq
    stats[t, 1:2, :] = cr

    def stat_copy(o, slot):
        return remote(stats.at[t], stats.at[slot], st_s.at[o], st_r.at[o], d, (t + o) % nt)

    for o in range(1, nt):
        stat_copy(o, t).start()
    for o in range(1, nt):
        stat_copy(o, (t - o + nt) % nt).wait_recv()
    sq = stats[0, 0:1, :]
    cr = stats[0, 1:2, :]
    for k in range(1, nt):
        sq = sq + stats[k, 0:1, :]
        cr = cr + stats[k, 1:2, :]
    features = feats * nt
    inv = 1.0 / jnp.sqrt(sq / features + epsilon)
    coef = inv * inv * inv * (cr / features)
    gt[...] = inv * sg[...] - coef * proj[...]
    gbuf[d] = jnp.transpose(gt[...]).astype(jnp.bfloat16)

    def g_copy(way, s):
        dd = {0: d - 2, 1: d + 2, 2: partner}[way]
        return remote(gbuf.at[s], gbuf.at[s], gs.at[way, s], gr.at[s], dd, t)

    @pl.when(z > 0)
    def _():
        g_copy(0, d).start()

    @pl.when(z < nz - 1)
    def _():
        g_copy(1, d).start()

    g_copy(2, d).start()

    def x_near(ct):
        for zt in range(nz):
            @pl.when((jnp.abs(z - zt) <= near) & (z != zt))
            def _(zt=zt):
                x_whole(2 * zt + ct, d, d).start()

    x_near(0)

    side = t + 1 - 2 * (t % 2)
    across = t + 2 - 4 * ((t // 2) % 2)

    def pair(flip):
        first = side + flip * (across - side)
        return first, side + across - first

    def run(n):
        return pl.ds(pl.multiple_of(n * nstep, nstep), nstep)

    def block(who):
        return pl.ds(pl.multiple_of(who * rows, rows), rows)

    def rs_copy(n, k):
        first, second = pair(n % 2)
        src = (
            part.at[block(side + across - t), run(n)],
            part.at[block(first), run(n)],
            relay.at[:, run(n)],
        )[k]
        return remote(
            src, rsbuf.at[k, :, run(n)], rs_s.at[n, k], rs_r.at[n, k], d,
            second if k == 2 else first,
        )

    def share(n, carry):
        part[:, run(n)] = jnp.dot(
            gbuf[d], wv[:, run(n)], preferred_element_type=jnp.float32
        ).astype(jnp.bfloat16)
        rs_copy(n, 0).start()
        rs_copy(n, 1).start()
        return carry

    lax.fori_loop(0, nchunks, share, 0)

    def pass_on(n, carry):
        second = pair(n % 2)[1]
        rs_copy(n, 0).wait_recv()
        relay[:, run(n)] = (
            part[block(second), run(n)].astype(jnp.float32)
            + rsbuf[0, :, run(n)].astype(jnp.float32)
        ).astype(jnp.bfloat16)
        rs_copy(n, 2).start()
        return carry

    def f_copy(s, k, whose=None):
        cs = s % 2
        who = (side, across, pair(1 - cs)[0])[k]
        mine_or = (t, t, pair(cs)[0])[k] if whose is None else whose
        return remote(
            xbuf.at[s, block(mine_or)], xbuf.at[s, block(mine_or)],
            fs.at[s, k], fr.at[s, k], d, who,
        )

    def f_wait(s, k):
        f_copy(s, k, (side, across, side + across - t)[k]).wait_recv()

    def f_relay(dist):
        def one(i, carry):
            zs = z + (2 * (i // 2) - 1) * dist

            @pl.when((zs >= 0) & (zs < nz))
            def _():
                s = 2 * zs + i % 2
                f_wait(s, 0)
                f_wait(s, 1)
                f_copy(s, 2).start()

            return carry

        lax.fori_loop(0, 4, one, 0)

    for dist in range(nz - 1, near, -1):
        for zs_of in (lambda: z - dist, lambda: z + dist):
            zs = zs_of()

            @pl.when((zs >= 0) & (zs < nz))
            def _(zs=zs):
                for cs in range(2):
                    s = 2 * zs + cs
                    x_share(d, s, s).wait_recv()
                    f_copy(s, 0).start()
                    f_copy(s, 1).start()

    def chain(k):
        @pl.when(z - k >= 0)
        def _():
            s = 2 * (z - k) + c
            g_copy(1, s).wait_recv()

            @pl.when(z < nz - 1)
            def _():
                g_copy(1, s).start()

            g_copy(2, s).start()

        @pl.when(z + k < nz)
        def _():
            s = 2 * (z + k) + c
            g_copy(0, s).wait_recv()

            @pl.when(z > 0)
            def _():
                g_copy(0, s).start()

            g_copy(2, s).start()

    def accumulate(s):
        wg_ref[...] += lax.dot_general(
            xbuf[s], gbuf[s], (((0,), (0,)), ((), ())), preferred_element_type=jnp.float32
        )

    def weight_terms(k):
        def one(i, carry):
            zs = z + (2 * (i // 2) - 1) * k
            cs = i % 2

            @pl.when((zs >= 0) & (zs < nz))
            def _():
                s = 2 * zs + cs
                if k <= near:
                    x_whole(d, s, s).wait_recv()
                else:
                    f_wait(s, 2)

                @pl.when(cs != c)
                def _():
                    g_copy(2, s).wait_recv()

                accumulate(s)

            return carry

        lax.fori_loop(0, 4, one, 0)

    own = pltpu.make_async_copy(x_hbm.at[:, col_block(d)], xbuf.at[d], lsem.at[2])
    own.start()
    chain(1)
    lax.fori_loop(0, nchunks // 2, pass_on, 0)
    x_near(1)
    own.wait()
    wg_ref[...] = jnp.zeros_like(wg_ref)
    accumulate(d)
    x_whole(d, partner, partner).wait_recv()
    g_copy(2, partner).wait_recv()
    accumulate(partner)
    lax.fori_loop(nchunks // 2, nchunks, pass_on, 0)
    for k in range(2, nz):
        chain(k)
        for dist in range(nz - 1, near, -1):
            if k == 2:
                f_relay(dist)
        weight_terms(k - 1)

    def total(n, carry):
        rs_copy(n, 1).wait_recv()
        rs_copy(n, 2).wait_recv()
        acc = part[mine, run(n)].astype(jnp.float32)
        for k in (1, 2):
            acc = acc + rsbuf[k, :, run(n)].astype(jnp.float32)
        ig_ref[:, run(n)] = acc.astype(jnp.bfloat16)
        return carry

    lax.fori_loop(0, nchunks, total, 0)
    weight_terms(nz - 1)

    for o in range(1, nt):
        stat_copy(o, t).wait_send()
    for zt in range(nz):
        for ct in range(2):
            s = 2 * zt + ct

            @pl.when(jnp.abs(z - zt) > near)
            def _(s=s):
                x_share(s, d, d).wait_send()
                for k in range(3):
                    f_copy(s, k).wait_send()

            @pl.when((jnp.abs(z - zt) <= near) & (z != zt))
            def _(s=s):
                x_whole(s, d, d).wait_send()

        s = 2 * zt + c

        @pl.when((zt >= z) & (z > 0))
        def _(s=s):
            g_copy(0, s).wait_send()

        @pl.when((zt <= z) & (z < nz - 1))
        def _(s=s):
            g_copy(1, s).wait_send()

        g_copy(2, s).wait_send()
    x_whole(partner, d, d).wait_send()

    def sent(n, carry):
        for k in range(3):
            rs_copy(n, k).wait_send()
        return carry

    lax.fori_loop(0, nchunks, sent, 0)


def write_out(ig_ref, wg_ref, ig_hbm, wg_hbm, sem):
    copies = (
        pltpu.make_async_copy(ig_ref, ig_hbm, sem.at[0]),
        pltpu.make_async_copy(wg_ref, wg_hbm, sem.at[1]),
    )
    for copy in copies:
        copy.start()
    for copy in copies:
        copy.wait()


def fused(block_input, query_weight, query_gain, query_grad):
    ndp = lax.axis_size("dp")
    nt = lax.axis_size("tensor")
    tokens, width = block_input.shape
    feats = query_weight.shape[0]
    cols, rows = width // ndp, tokens // nt
    fchunks, nchunks = 2, 4
    dma = pltpu.SemaphoreType.DMA
    bf, f32 = jnp.bfloat16, jnp.float32
    hbm = pl.BlockSpec(memory_space=pltpu.HBM)
    vmem = pl.BlockSpec(memory_space=pltpu.VMEM)
    outs = pl.pallas_call(
        functools.partial(kernel, ndp, nt, fchunks, nchunks, 1),
        out_shape=(
            pltpu.VMEM((rows, width), bf),
            pltpu.VMEM((cols, feats), f32),
        ),
        in_specs=[hbm, hbm, hbm, vmem],
        out_specs=(vmem, vmem),
        scratch_shapes=[
            pltpu.VMEM((tokens, width), bf),
            pltpu.VMEM((feats, width), bf),
            pltpu.VMEM((feats, tokens), bf),
            pltpu.VMEM((feats, tokens), f32),
            pltpu.VMEM((feats, tokens), f32),
            pltpu.VMEM((nt, 8, tokens), f32),
            pltpu.VMEM((feats, tokens), f32),
            pltpu.VMEM((ndp, tokens, feats), bf),
            pltpu.VMEM((ndp, tokens, cols), bf),
            pltpu.VMEM((tokens, width), bf),
            pltpu.VMEM((3, rows, width), bf),
            pltpu.VMEM((rows, width), bf),
            dma((3,)), dma((fchunks,)),
            dma((nt,)), dma((nt,)),
            dma((ndp,)), dma((ndp,)),
            dma((ndp, 3)), dma((ndp, 3)),
            dma((3, ndp)), dma((ndp,)),
            dma((nchunks, 3)), dma((nchunks, 3)),
        ],
        compiler_params=pltpu.CompilerParams(
            collective_id=0, has_side_effects=True, vmem_limit_bytes=64 * 1024 * 1024 - 2560 * 1024
        ),
        name="query_backward",
    )(block_input, query_weight, query_grad, query_gain)
    return pl.pallas_call(
        write_out,
        out_shape=tuple(jax.ShapeDtypeStruct(o.shape, o.dtype) for o in outs),
        in_specs=[vmem, vmem],
        out_specs=(hbm, hbm),
        scratch_shapes=[dma((2,))],
        compiler_params=pltpu.CompilerParams(vmem_limit_bytes=8 * 1024 * 1024),
        name="write_out",
    )(*outs)


def per_device(block_input, query_weight, query_gain, query_grad):
    ndp = lax.axis_size("dp")
    nt = lax.axis_size("tensor")
    tokens, width = block_input.shape
    feats = query_weight.shape[0]
    aligned = (
        ndp % 2 == 0 and ndp >= 6 and nt == 4
        and width % (128 * ndp) == 0 and width % (128 * 4) == 0
        and feats % 128 == 0 and tokens % 128 == 0 and tokens % (16 * nt) == 0
        and 2 * width * (feats + 4 * tokens) + 24 * tokens * feats < 40 * 2**20
    )
    body = fused if aligned else plain
    return body(block_input, query_weight, query_gain, query_grad)


def solution(mesh):
    in_specs = (P("dp", None), P("tensor", None), P("tensor"), P("tensor", "dp"))
    out_specs = (P(("dp", "tensor"), None), P("dp", "tensor"))
    return jax.shard_map(
        per_device, mesh=mesh, in_specs=in_specs, out_specs=out_specs, check_vma=False
    )
```
